32 devices in a mesh: clip: 4 (over z), seq: 4 (over x, core), head: 2 (over y).
Axes of the slice: x: 2, y: 2, z: 4, core: 2. Of those that a mesh axis runs over, the one named last changes fastest.
Arguments:
- inputs: float32 [4, 16, 196, 768], P('clip', 'seq'), may hold values from -39 to 39, as said below
- space_gain: float32 [768], P(('clip', 'seq')), may hold values from 0.5 to 1.5
- space_shift: float32 [768], P(('clip', 'seq')), may hold values from -3 to 3
- space_proj: float32 [768, 3, 768], P(('clip', 'seq'), None, 'head'), may hold values from -0.3125 to 0.3125
- space_bias: float32 [2, 6, 128], P(None, 'head', ('clip', 'seq')), may hold values from -3 to 3
- space_out: float32 [768, 768], P('head', ('clip', 'seq')), may hold values from -0.875 to 0.875
- space_out_bias: float32 [768], P(('clip', 'seq')), may hold values from -3 to 3
- time_gain: float32 [768], P(('clip', 'seq')), may hold values from 0.5 to 1.5
- time_shift: float32 [768], P(('clip', 'seq')), may hold values from -3 to 3
- time_proj: float32 [768, 3, 768], P(('clip', 'seq'), None, 'head'), may hold values from -0.3125 to 0.3125
- time_bias: float32 [2, 6, 128], P(None, 'head', ('clip', 'seq')), may hold values from -3 to 3
- time_out: float32 [768, 768], P('head', ('clip', 'seq')), may hold values from -0.4375 to 0.4375
- time_out_bias: float32 [768], P(('clip', 'seq')), may hold values from -3 to 3
- dense_gain: float32 [768], P(('clip', 'seq')), may hold values from 0.5 to 1.5
- dense_shift: float32 [768], P(('clip', 'seq')), may hold values from -3 to 3
- dense_in: float32 [768, 3072], P(('clip', 'seq'), 'head'), may hold values from -0.21875 to 0.21875
- dense_bias: float32 [24, 128], P('head', ('clip', 'seq')), may hold values from -3 to 3
- dense_out: float32 [3072, 768], P('head', ('clip', 'seq')), may hold values from -0.15625 to 0.15625
- dense_out_bias: float32 [768], P(('clip', 'seq')), may hold values from -3 to 3
- cotangent: float32 [4, 16, 196, 768], P('clip', 'seq'), may hold values from -6 to 6
Outputs:
- outputs: float32 [4, 16, 196, 768], P('clip', 'seq')
- input_grad: float32 [4, 16, 196, 768], P('clip', 'seq')
- grad_space_gain: float32 [768], P(('clip', 'seq'))
- grad_space_shift: float32 [768], P(('clip', 'seq'))
- grad_space_proj: float32 [768, 3, 768], P(('clip', 'seq'), None, 'head')
- grad_space_bias: float32 [2, 6, 128], P(None, 'head', ('clip', 'seq'))
- grad_space_out: float32 [768, 768], P('head', ('clip', 'seq'))
- grad_space_out_bias: float32 [768], P(('clip', 'seq'))
- grad_time_gain: float32 [768], P(('clip', 'seq'))
- grad_time_shift: float32 [768], P(('clip', 'seq'))
- grad_time_proj: float32 [768, 3, 768], P(('clip', 'seq'), None, 'head')
- grad_time_bias: float32 [2, 6, 128], P(None, 'head', ('clip', 'seq'))
- grad_time_out: float32 [768, 768], P('head', ('clip', 'seq'))
- grad_time_out_bias: float32 [768], P(('clip', 'seq'))
- grad_dense_gain: float32 [768], P(('clip', 'seq'))
- grad_dense_shift: float32 [768], P(('clip', 'seq'))
- grad_dense_in: float32 [768, 3072], P(('clip', 'seq'), 'head')
- grad_dense_bias: float32 [24, 128], P('head', ('clip', 'seq'))
- grad_dense_out: float32 [3072, 768], P('head', ('clip', 'seq'))
- grad_dense_out_bias: float32 [768], P(('clip', 'seq'))
The draws below stay inside these ranges and needn't reach their ends.
Inputs may be any that keep to these rules, and one draw needn't show every extreme that they name: `inputs`: real token features.
All inputs are finite; a program needn't handle non-finite values.
Results may differ from the reference program's by a relative error of at most 0.029.
Values may be sent and summed in bfloat16 or wider, within the bound.
A program may use at most 128 MiB of HBM per device.

```python
import math
import jax
import jax.numpy as jnp
from jax import lax

D = 768
HEADS = 12
HEAD_DIM = 64
FF = 3072
FRAMES = 16
PLACES = 196
CLIPS = 4
N_HEAD = 2


def draw_inputs(key, part):
    key_base, key_rows, key_cols = jax.random.split(key, 3)
    full_shape = (CLIPS, FRAMES, PLACES, D)
    row_scale = jnp.exp(jax.random.uniform(key_rows, (CLIPS, FRAMES, PLACES, 1), jnp.float32, math.log(0.3), math.log(3.0)))
    column_scale = jnp.exp(jax.random.uniform(key_cols, (1, 1, 1, D), jnp.float32, math.log(0.3), math.log(3.0)))
    entries = jnp.clip(jax.random.normal(key_base, full_shape, jnp.float32), -4.0, 4.0)
    return entries * row_scale * column_scale


def strengthened(array, own_key, source, target, shards_of, factor):
    owner, partner = [(jnp.arange(array.shape[position]) // (array.shape[position] // shards_of)).reshape([-1 if axis == position else 1 for axis in range(array.ndim)]) for position in (source, target)]
    chosen = jax.random.permutation(own_key, shards_of)[partner]
    strong = (owner == chosen) | (owner == (partner + shards_of // 2) % shards_of)
    return jnp.where(strong, factor * array, array)


def level_of(own_key, shape, cuts, least, high):
    def one(axis_at, shards_of):
        heights = jax.random.uniform(jax.random.fold_in(jax.random.fold_in(own_key, 6), axis_at), (shards_of,), jnp.float32, least / len(cuts), high / len(cuts))
        return jnp.repeat(jnp.exp(heights), shape[axis_at] // shards_of).reshape((-1,) + (1,) * (len(shape) - axis_at - 1))

    gain = one(*cuts[0])
    for cut in cuts[1:]:
        gain = gain * one(*cut)
    return gain


def gaussian(stream_key, shape, width, bound, cuts=(), kind=jnp.bfloat16):
    level = level_of(stream_key, shape, cuts, -0.22, 0.18) if cuts else 1.0
    values = jax.random.normal(stream_key, shape, jnp.float32) * width * level
    return jnp.minimum(jnp.maximum(values, -bound), bound).astype(kind)


def heavy_noise(key, dims, scale, reach, pieces, heavy, kind=jnp.bfloat16):
    values = scale * jax.random.normal(key, dims, jnp.float32)
    if pieces:
        values = values * level_of(key, dims, pieces, -0.22, 0.18)
    return jnp.clip(strengthened(values, jax.random.fold_in(key, 3), *heavy), -reach, reach).astype(kind)


def setup_inputs(seed: int = 0) -> dict:
    seeds = jax.random.split(jax.random.key(seed), 21)
    inputs = draw_inputs(jax.random.fold_in(seeds[20], 71), 0)
    space_gain = jnp.clip(1.0 + 0.1 * jax.random.normal(seeds[1], (D,), jnp.float32), 0.5, 1.5)
    space_shift = gaussian(seeds[2], (D,), 0.5, 3.0, ((0, 16),), jnp.float32)
    space_proj = gaussian(seeds[3], (D, 3, D), (D // 2) ** -0.5, 0.3125, ((0, 16), (2, 2)), jnp.float32)
    space_bias = gaussian(seeds[4], (2, D // 128, 128), 0.5, 3.0, ((1, 2), (2, 16)), jnp.float32)
    space_out = gaussian(seeds[5], (D, D), (D // 16) ** -0.5, 0.875, ((0, 2), (1, 16)), jnp.float32)
    space_out_bias = gaussian(seeds[6], (D,), 0.5, 3.0, ((0, 16),), jnp.float32)
    time_gain = jnp.clip(1.0 + 0.1 * jax.random.normal(seeds[7], (D,), jnp.float32), 0.5, 1.5)
    time_shift = gaussian(seeds[8], (D,), 0.5, 3.0, ((0, 16),), jnp.float32)
    time_proj = gaussian(seeds[9], (D, 3, D), (D // 2) ** -0.5, 0.3125, ((0, 16), (2, 2)), jnp.float32)
    time_bias = gaussian(seeds[10], (2, D // 128, 128), 0.5, 3.0, ((1, 2), (2, 16)), jnp.float32)
    time_out = gaussian(seeds[11], (D, D), (D // 4) ** -0.5, 0.4375, ((0, 2), (1, 16)), jnp.float32)
    time_out_bias = gaussian(seeds[12], (D,), 0.5, 3.0, ((0, 16),), jnp.float32)
    dense_gain = jnp.clip(1.0 + 0.1 * jax.random.normal(seeds[13], (D,), jnp.float32), 0.5, 1.5)
    dense_shift = gaussian(seeds[14], (D,), 0.5, 3.0, ((0, 16),), jnp.float32)
    dense_in = gaussian(seeds[15], (D, FF), D ** -0.5, 0.21875, ((0, 16), (1, 2)), jnp.float32)
    dense_bias = gaussian(seeds[16], (FF // 128, 128), 0.5, 3.0, ((0, 2), (1, 16)), jnp.float32)
    dense_out = gaussian(seeds[17], (FF, D), (FF // 2) ** -0.5, 0.15625, ((0, 2), (1, 16)), jnp.float32)
    dense_out_bias = gaussian(seeds[18], (D,), 0.5, 3.0, ((0, 16),), jnp.float32)
    cotangent = heavy_noise(seeds[19], (CLIPS, FRAMES, PLACES, D), 1.0, 6.0, ((0, 4), (1, 4)), (0, 3, 4, 2.0), jnp.float32)
    return {"inputs": inputs, "space_gain": space_gain, "space_shift": space_shift, "space_proj": space_proj, "space_bias": space_bias, "space_out": space_out, "space_out_bias": space_out_bias, "time_gain": time_gain, "time_shift": time_shift, "time_proj": time_proj, "time_bias": time_bias, "time_out": time_out, "time_out_bias": time_out_bias, "dense_gain": dense_gain, "dense_shift": dense_shift, "dense_in": dense_in, "dense_bias": dense_bias, "dense_out": dense_out, "dense_out_bias": dense_out_bias, "cotangent": cotangent}


norm_eps = 1e-06
HIGHEST = lax.Precision.HIGHEST

@jax.custom_vjp
def low(v):
    return lax.optimization_barrier(v.astype(jnp.bfloat16)).astype(jnp.float32)

@jax.custom_vjp
def low_back(v):
    return v

def low_keep(v):
    return (low(v), None)

def low_pass(kept, grad):
    return (grad,)

def back_keep(v):
    return (v, None)

def back_low(kept, grad):
    return (low(grad),)
low.defvjp(low_keep, low_pass)
low_back.defvjp(back_keep, back_low)

def rounded_both(values):
    return low_back(low(values))

def layer_norm(values, norm_gain, norm_shift):
    row_mean = lax.optimization_barrier(jnp.mean(values, axis=-1, keepdims=True))
    centred = values - row_mean
    spread = lax.optimization_barrier(jnp.mean(centred * centred, axis=-1, keepdims=True))
    return centred * lax.rsqrt(spread + norm_eps) * norm_gain + norm_shift

def attention(merged_rows, letters):
    query_form, key_form, score_form = letters
    queries = merged_rows[..., 0, :, :]
    key_rows = merged_rows[..., 1, :, :]
    value_rows = merged_rows[..., 2, :, :]
    raw_scores = jnp.einsum(query_form + ',' + key_form + '->' + score_form, queries, key_rows, precision=HIGHEST)
    scores = low_back(raw_scores * HEAD_DIM ** (-0.5))
    attn_probs = low(jax.nn.softmax(scores, axis=-1))
    return rounded_both(jnp.einsum(score_form + ',' + key_form + '->' + query_form, attn_probs, value_rows, precision=HIGHEST))

def attention_block(stream, norm_gain, norm_shift, proj, bias, out_proj, out_bias, letters):
    normed = low(layer_norm(stream, norm_gain, norm_shift))
    local_width = D // N_HEAD
    local_heads = HEADS // N_HEAD
    bias_rows = bias.reshape(2, D)
    bias_full = jnp.stack([bias_rows[0], jnp.zeros((D,), jnp.float32), bias_rows[1]])
    branch = jnp.zeros(stream.shape, jnp.float32)
    for member in range(N_HEAD):
        start_col = member * local_width
        columns = proj[:, :, start_col:start_col + local_width]
        merged_rows = jnp.einsum('fpd,dkj->fpkj', low_back(normed), columns, precision=HIGHEST) + bias_full[:, start_col:start_col + local_width]
        merged_rows = rounded_both(merged_rows).reshape(FRAMES, PLACES, 3, local_heads, HEAD_DIM)
        mixed_rows = attention(merged_rows, letters).reshape(FRAMES, PLACES, local_width)
        branch = branch + low(jnp.einsum('fpw,wd->fpd', mixed_rows, out_proj[start_col:start_col + local_width], precision=HIGHEST))
    return stream + low_back(branch) + out_bias

def dense_block(stream, norm_gain, norm_shift, proj_in, bias_in, proj_out, out_bias):
    normed = low(layer_norm(stream, norm_gain, norm_shift))
    local_hidden = FF // N_HEAD
    bias_flat = bias_in.reshape(FF)
    branch = jnp.zeros(stream.shape, jnp.float32)
    for member in range(N_HEAD):
        start_col = member * local_hidden
        product_rows = jnp.einsum('fpd,dh->fph', low_back(normed), proj_in[:, start_col:start_col + local_hidden], precision=HIGHEST)
        pre_rows = low_back(product_rows) + bias_flat[start_col:start_col + local_hidden]
        act_rows = rounded_both(jax.nn.gelu(pre_rows, approximate=False))
        branch = branch + low(jnp.einsum('fph,hd->fpd', act_rows, proj_out[start_col:start_col + local_hidden], precision=HIGHEST))
    return stream + low_back(branch) + out_bias

def forward(clip_rows, params):
    lowered = [low(master) for master in params]
    after_space = attention_block(clip_rows, *lowered[0:6], ('fphe', 'fqhe', 'fhpq'))
    after_time = attention_block(after_space, *lowered[6:12], ('fphe', 'gphe', 'phfg'))
    return dense_block(after_time, *lowered[12:18])

def reference(inputs, space_gain, space_shift, space_proj, space_bias, space_out, space_out_bias, time_gain, time_shift, time_proj, time_bias, time_out, time_out_bias, dense_gain, dense_shift, dense_in, dense_bias, dense_out, dense_out_bias, cotangent):
    params = (space_gain, space_shift, space_proj, space_bias, space_out, space_out_bias, time_gain, time_shift, time_proj, time_bias, time_out, time_out_bias, dense_gain, dense_shift, dense_in, dense_bias, dense_out, dense_out_bias)

    def clip_step(totals, clip_pair):
        clip_rows, clip_grad = clip_pair
        outcome, pullback = jax.vjp(forward, clip_rows, params)
        grad_clip, grad_params = pullback(clip_grad)
        return (jax.tree.map(jnp.add, totals, grad_params), (outcome, grad_clip))
    start_totals = jax.tree.map(jnp.zeros_like, params)
    totals, (outputs, input_grad) = lax.scan(clip_step, start_totals, (inputs, cotangent))
    return (outputs, input_grad, totals[0], totals[1], totals[2], totals[3], totals[4], totals[5], totals[6], totals[7], totals[8], totals[9], totals[10], totals[11], totals[12], totals[13], totals[14], totals[15], totals[16], totals[17])
```

```python
import jax
import jax.numpy as jnp
from jax import lax
from jax.sharding import PartitionSpec as P

HEAD_DIM = 64
NORM_EPS = 1e-06
BF = jnp.bfloat16
F32 = jnp.float32
SHARDS = ("head", "clip", "seq")
PLACE_AXES = ("seq", "head")


def product(form, left, right):
    return jnp.einsum(form, left, right, preferred_element_type=F32)


def norm_stats(values):
    mean = jnp.mean(values, axis=-1, keepdims=True)
    centred = values - mean
    spread = jnp.mean(centred * centred, axis=-1, keepdims=True)
    rate = lax.rsqrt(spread + NORM_EPS)
    return centred * rate, rate


def norm_back(unit, rate, gain, grad_normed):
    grad_gain = jnp.sum(grad_normed * unit, axis=0)
    grad_shift = jnp.sum(grad_normed, axis=0)
    scaled = grad_normed * gain
    inner = jnp.mean(scaled * unit, axis=-1, keepdims=True)
    outer = jnp.mean(scaled, axis=-1, keepdims=True)
    return rate * (scaled - outer - unit * inner), grad_gain, grad_shift


def project_in(normed, weights, bias):
    groups, _, triple = weights.shape
    width = triple // 3
    full = jnp.stack([bias[:, 0], jnp.zeros_like(bias[:, 0]), bias[:, 1]], axis=1)
    rows = product("nd,hdk->hnk", normed, weights) + full.reshape(groups, 1, triple)
    return rows.astype(BF).reshape(groups, normed.shape[0], 3, width)


def split_heads(merged, lead):
    groups = merged.shape[0]
    shaped = merged.reshape((groups,) + lead + (3, merged.shape[-1] // HEAD_DIM, HEAD_DIM))
    return shaped[..., 0, :, :], shaped[..., 1, :, :], shaped[..., 2, :, :]


def attend(merged, lead):
    queries, keys, values = split_heads(merged, lead)
    scores = product("gbqje,gbkje->gbjqk", queries, keys) * HEAD_DIM ** (-0.5)
    weights = jnp.exp(scores - jnp.max(scores, axis=-1, keepdims=True))
    probs = weights / jnp.sum(weights, axis=-1, keepdims=True)
    mixed = product("gbjqk,gbkje->gbqje", probs.astype(BF), values).astype(BF)
    return mixed.reshape(merged.shape[0], merged.shape[1], merged.shape[3]), probs


def attend_back(merged, probs, grad_mixed, lead):
    queries, keys, values = split_heads(merged, lead)
    grad_heads = grad_mixed.reshape(queries.shape)
    grad_values = product("gbjqk,gbqje->gbkje", probs.astype(BF), grad_heads)
    grad_probs = product("gbqje,gbkje->gbjqk", grad_heads, values)
    grad_scores = probs * (grad_probs - jnp.sum(probs * grad_probs, axis=-1, keepdims=True))
    grad_scores = grad_scores.astype(BF)
    scale = HEAD_DIM ** (-0.5)
    grad_queries = product("gbjqk,gbkje->gbqje", grad_scores, keys) * scale
    grad_keys = product("gbjqk,gbqje->gbkje", grad_scores, queries) * scale
    stacked = jnp.stack([grad_queries, grad_keys, grad_values], axis=3).astype(BF)
    return stacked.reshape(merged.shape)


def to_places(rows, count):
    frames, places, width = rows.shape
    share = -(-places // count)
    padded = jnp.pad(rows, ((0, 0), (0, share * count - places), (0, 0)))
    cut = padded.reshape(frames, count, share, width).transpose(1, 0, 2, 3)
    moved = lax.all_to_all(cut, PLACE_AXES, split_axis=0, concat_axis=0, tiled=True)
    return moved.reshape(count * frames, share, width)


def to_frames(rows, count, places):
    total, share, width = rows.shape
    frames = total // count
    cut = rows.reshape(count, frames, share, width)
    moved = lax.all_to_all(cut, PLACE_AXES, split_axis=0, concat_axis=0, tiled=True)
    back = moved.transpose(1, 0, 2, 3).reshape(frames, count * share, width)
    return back[:, :places]


def gather(block):
    return lax.all_gather(block, SHARDS, axis=0, tiled=False)


def body(
    inputs,
    space_gain,
    space_shift,
    space_proj,
    space_bias,
    space_out,
    space_out_bias,
    time_gain,
    time_shift,
    time_proj,
    time_bias,
    time_out,
    time_out_bias,
    dense_gain,
    dense_shift,
    dense_in,
    dense_bias,
    dense_out,
    dense_out_bias,
    cotangent,
):
    n_head = lax.axis_size("head")
    n_own = lax.axis_size("clip") * lax.axis_size("seq")
    count = lax.axis_size("seq") * n_head
    here = lax.axis_index("head")
    _, held, places, width = inputs.shape
    frames = held // n_head
    strip = space_gain.shape[0]

    def block_of(proj, out):
        flat = proj.reshape(strip, -1).astype(BF)
        return jnp.concatenate([flat, out.astype(BF).T], axis=1)

    def whole(block):
        return gather(block).reshape(n_head, width, block.shape[1])

    space_all = whole(block_of(space_proj, space_out))
    time_all = whole(block_of(time_proj, time_out))
    dense_all = whole(block_of(dense_in, dense_out))
    part = space_out.shape[0]
    hidden = dense_out.shape[0]

    vectors = (
        space_gain, space_shift, space_out_bias, time_gain, time_shift, time_out_bias,
        dense_gain, dense_shift, dense_out_bias,
    )
    odd = (space_bias, time_bias, dense_bias)
    small = jnp.concatenate([v.reshape(-1) for v in vectors + odd]).astype(BF)
    small_all = gather(small).reshape(n_head, n_own, -1).astype(F32)
    whole_vectors = []
    for i in range(len(vectors)):
        whole_vectors.append(small_all[0, :, i * strip:(i + 1) * strip].reshape(width))
    at = len(vectors) * strip
    sizes = [v.size for v in odd]
    bias_s = small_all[:, :, at:at + sizes[0]]
    bias_t = small_all[:, :, at + sizes[0]:at + sizes[0] + sizes[1]]
    bias_d = small_all[:, :, at + sizes[0] + sizes[1]:]

    def rows_bias(flat, shape):
        lines, lanes = shape[:-1], shape[-1]
        count_lines = 1
        for n in lines:
            count_lines *= n
        spread = flat.reshape(n_head, n_own, count_lines, lanes).transpose(0, 2, 1, 3)
        return spread.reshape(n_head, lines[0], -1)

    bias_s = rows_bias(bias_s, space_bias.shape)
    bias_t = rows_bias(bias_t, time_bias.shape)
    bias_d = rows_bias(bias_d, dense_bias.shape).reshape(n_head, 1, hidden)
    (g_s, b_s, ob_s, g_t, b_t, ob_t, g_d, b_d, ob_d) = whole_vectors

    own = lax.dynamic_slice_in_dim(inputs[0], here * frames, frames, axis=0)
    own = own.reshape(frames * places, width)
    cot = lax.dynamic_slice_in_dim(cotangent[0], here * frames, frames, axis=0)
    cot = cot.reshape(frames * places, width)

    proj_s, out_s = space_all[..., :3 * part], space_all[..., 3 * part:]
    proj_t, out_t = time_all[..., :3 * part], time_all[..., 3 * part:]
    in_d, out_d = dense_all[..., :hidden], dense_all[..., hidden:]

    unit_s, rate_s = norm_stats(own)
    normed_s = (unit_s * g_s + b_s).astype(BF)
    merged_s = project_in(normed_s, proj_s, bias_s)
    mixed_s, probs_s = attend(merged_s, (frames, places))
    after_space = own + product("hnw,hdw->nd", mixed_s, out_s) + ob_s

    unit_t, rate_t = norm_stats(after_space)
    normed_t = (unit_t * g_t + b_t).astype(BF)
    rows_t = to_places(normed_t.reshape(frames, places, width), count)
    total_frames, share = rows_t.shape[:2]
    rows_t = rows_t.transpose(1, 0, 2).reshape(-1, width)
    lead_t = (share, total_frames)
    merged_t = project_in(rows_t, proj_t, bias_t)
    mixed_t, probs_t = attend(merged_t, lead_t)
    branch_t = product("hnw,hdw->nd", mixed_t, out_t).astype(BF)
    branch_t = to_frames(branch_t.reshape(share, total_frames, width).transpose(1, 0, 2), count, places)
    after_time = after_space + branch_t.reshape(-1, width).astype(F32) + ob_t

    unit_d, rate_d = norm_stats(after_time)
    normed_d = (unit_d * g_d + b_d).astype(BF)
    pre = product("nd,hdk->hnk", normed_d, in_d) + bias_d
    act = jax.nn.gelu(pre, approximate=False).astype(BF)
    result = after_time + product("hnk,hdk->nd", act, out_d) + ob_d

    grad_ob_d = jnp.sum(cot, axis=0)
    low_d = cot.astype(BF)
    grad_out_d = product("nd,hnk->hdk", low_d, act)
    grad_act = product("nd,hdk->hnk", low_d, out_d).astype(BF).astype(F32)
    _, pull = jax.vjp(lambda v: jax.nn.gelu(v, approximate=False), pre)
    grad_pre = pull(grad_act)[0]
    grad_bias_d = jnp.sum(grad_pre, axis=1)
    low_pre = grad_pre.astype(BF)
    grad_in_d = product("nd,hnk->hdk", normed_d, low_pre)
    grad_normed = product("hnk,hdk->nd", low_pre, in_d)
    grad_v, grad_g_d, grad_b_d = norm_back(unit_d, rate_d, g_d, grad_normed)
    stream_t = cot + grad_v

    grad_ob_t = jnp.sum(stream_t, axis=0)
    low_t = to_places(stream_t.astype(BF).reshape(frames, places, width), count)
    low_t = low_t.transpose(1, 0, 2).reshape(-1, width)
    grad_out_t = product("nd,hnw->hdw", low_t, mixed_t)
    grad_mixed = product("nd,hdw->hnw", low_t, out_t).astype(BF)
    grad_merged_t = attend_back(merged_t, probs_t, grad_mixed, lead_t)
    sums_t = jnp.sum(grad_merged_t.astype(F32), axis=1)
    flat_t = grad_merged_t.reshape(n_head, -1, 3 * part)
    grad_proj_t = product("nd,hnk->hdk", rows_t, flat_t)
    grad_rows = product("hnk,hdk->nd", flat_t, proj_t).astype(BF)
    grad_rows = to_frames(grad_rows.reshape(share, total_frames, width).transpose(1, 0, 2), count, places)
    grad_v, grad_g_t, grad_b_t = norm_back(unit_t, rate_t, g_t, grad_rows.reshape(-1, width).astype(F32))
    stream_s = stream_t + grad_v

    grad_ob_s = jnp.sum(stream_s, axis=0)
    low_s = stream_s.astype(BF)
    grad_out_s = product("nd,hnw->hdw", low_s, mixed_s)
    grad_mixed = product("nd,hdw->hnw", low_s, out_s).astype(BF)
    grad_merged_s = attend_back(merged_s, probs_s, grad_mixed, (frames, places))
    sums_s = jnp.sum(grad_merged_s.astype(F32), axis=1)
    flat_s = grad_merged_s.reshape(n_head, -1, 3 * part)
    grad_proj_s = product("nd,hnk->hdk", normed_s, flat_s)
    grad_rows = product("hnk,hdk->nd", flat_s, proj_s)
    grad_v, grad_g_s, grad_b_s = norm_back(unit_s, rate_s, g_s, grad_rows)
    input_own = stream_s + grad_v

    def owners(proj_grad, out_grad):
        both = jnp.concatenate([proj_grad.astype(BF), out_grad.astype(BF)], axis=2)
        mine = lax.psum_scatter(both.reshape(n_head * width, -1), SHARDS, scatter_dimension=0, tiled=True)
        return mine.astype(F32)

    own_d = owners(grad_in_d, grad_out_d)
    own_t = owners(grad_proj_t, grad_out_t)
    own_s = owners(grad_proj_s, grad_out_s)

    vector_grads = jnp.stack([
        grad_g_s, grad_b_s, grad_ob_s, grad_g_t, grad_b_t, grad_ob_t, grad_g_d, grad_b_d, grad_ob_d,
    ])
    vector_grads = vector_grads.reshape(-1, n_own, strip).transpose(1, 0, 2).reshape(n_own, -1)

    def spread_bias(rows, shape):
        lanes = shape[-1]
        cut = rows.reshape(n_head, -1, n_own, lanes).transpose(0, 2, 1, 3)
        return cut.reshape(n_head, n_own, -1)

    odd_grads = jnp.concatenate([
        spread_bias(sums_s[:, ::2], space_bias.shape),
        spread_bias(sums_t[:, ::2], time_bias.shape),
        spread_bias(grad_bias_d, dense_bias.shape),
    ], axis=2)
    both = jnp.concatenate([vector_grads, odd_grads.transpose(1, 0, 2).reshape(n_own, -1)], axis=1)
    mine = lax.psum_scatter(both, ("clip", "seq"), scatter_dimension=0, tiled=True)
    mine = lax.psum(mine, "head")[0]
    got = [mine[i * strip:(i + 1) * strip] for i in range(9)]
    rest = mine[9 * strip:].reshape(n_head, -1)
    rest = lax.dynamic_index_in_dim(rest, here, axis=0, keepdims=False)
    odd_got = []
    at = 0
    for v in odd:
        odd_got.append(rest[at:at + v.size].reshape(v.shape))
        at += v.size

    def share_rows(rows):
        low = rows.astype(BF).reshape(frames, places, width)
        both_rows = lax.all_gather(low, "head", axis=0, tiled=True)
        return both_rows.astype(F32)[None]

    return (
        share_rows(result),
        share_rows(input_own),
        got[0],
        got[1],
        own_s[:, :3 * part].reshape(space_proj.shape),
        odd_got[0],
        own_s[:, 3 * part:].T,
        got[2],
        got[3],
        got[4],
        own_t[:, :3 * part].reshape(time_proj.shape),
        odd_got[1],
        own_t[:, 3 * part:].T,
        got[5],
        got[6],
        got[7],
        own_d[:, :hidden],
        odd_got[2],
        own_d[:, hidden:].T,
        got[8],
    )


def solution(mesh):
    both = ("clip", "seq")
    rows = P("clip", "seq", None, None)
    vec = P(both)
    weights = (
        vec, vec, P(both, None, "head"), P(None, "head", both), P("head", both), vec,
        vec, vec, P(both, None, "head"), P(None, "head", both), P("head", both), vec,
        vec, vec, P(both, "head"), P("head", both), P("head", both), vec,
    )
    return jax.shard_map(
        body,
        mesh=mesh,
        in_specs=(rows,) + weights + (rows,),
        out_specs=(rows, rows) + weights,
        check_vma=False,
    )
```

```python
import functools

import jax
import jax.numpy as jnp
from jax import lax
from jax.experimental import pallas as pl
from jax.experimental.pallas import tpu as pltpu
from jax.sharding import PartitionSpec as P


HEAD_DIM = 64
NORM_EPS = 1e-06
BF = jnp.bfloat16
F32 = jnp.float32
SHARDS = ("head", "clip", "seq")
PLACE_AXES = ("seq", "head")

MESH = pl.DeviceIdType.MESH


def position():
    seq = lax.axis_index("seq")
    return lax.axis_index("clip"), seq // 2, lax.rem(seq, 2), lax.axis_index("head")


def greet(n_clip, clip, side, core, head):
    barrier = pltpu.get_barrier_semaphore()
    peers = [{"seq": side * 2 + 1 - core}, {"seq": (1 - side) * 2 + core}, {"head": 1 - head}]
    for step in range(1, n_clip):
        peers.append({"clip": lax.rem(clip + step, n_clip)})
    for peer in peers:
        pl.semaphore_signal(barrier, inc=1, device_id=peer, device_id_type=MESH)
    pl.semaphore_wait(barrier, len(peers))


def scatter_kernel(n_clip, pieces, n_src, *refs):
    srcs, outs, scratch = refs[:n_src], refs[n_src:n_src + 2], refs[n_src + 2:]
    kinds = (scratch[0:5], scratch[5:10])
    sems = scratch[10]
    clip, side, core, head = position()
    greet(n_clip, clip, side, core, head)

    def send(src, dst, piece, kind, peer):
        return pltpu.make_async_remote_copy(
            src_ref=src, dst_ref=dst, send_sem=sems.at[0, piece, kind],
            recv_sem=sems.at[1, piece, kind], device_id=peer, device_id_type=MESH,
        )

    started = []
    firsts = []
    for i, (kind, slot, src, at, size, _) in enumerate(pieces):
        own, got = kinds[kind][0], kinds[kind][1]
        cols = pl.ds(at, size)
        pairs = []
        for b in range(2):
            away = send(
                srcs[src].at[:, :, b, 1 - core, :, cols], got.at[slot, :, b], i, b,
                {"seq": side * 2 + 1 - core},
            )
            away.start()
            near = pltpu.make_async_copy(
                srcs[src].at[:, :, b, core, :, cols], own.at[slot, :, b],
                sems.at[0, i, n_clip + 3 + b],
            )
            near.start()
            started.append(away)
            pairs.append((away, near))
        firsts.append(pairs)

    seconds, thirds, fourths = {}, {}, {}

    def add_into(own, got, dtype):
        own[...] = (own[...].astype(F32) + got[...].astype(F32)).astype(dtype)

    def first(i):
        kind, slot = pieces[i][:2]
        own, got, mid = kinds[kind][:3]
        for away, near in firsts[i]:
            near.wait()
            away.wait_recv()
        dtype = own.dtype

        def step(c, carry):
            for a in range(2):
                for b in range(2):
                    add_into(own.at[slot, a, b, c], got.at[slot, a, b, c], dtype)
            return carry

        lax.fori_loop(0, n_clip, step, 0)
        if i % 2 == 0:
            away = send(own.at[slot, 1 - head], mid.at[slot], i, 2, {"head": 1 - head})
        else:
            away = send(
                own.at[slot, :, 1 - side], mid.at[slot], i, 2,
                {"seq": (1 - side) * 2 + core},
            )
        away.start()
        started.append(away)
        seconds[i] = away

    def second(i):
        kind, slot = pieces[i][:2]
        own, _, mid, late = kinds[kind][:4]
        seconds[i].wait_recv()
        dtype = own.dtype
        if i % 2 == 0:
            def step(c, carry):
                for b in range(2):
                    add_into(own.at[slot, head, b, c], mid.at[slot, b, c], dtype)
                return carry

            lax.fori_loop(0, n_clip, step, 0)
            away = send(
                own.at[slot, head, 1 - side], late.at[slot], i, 3,
                {"seq": (1 - side) * 2 + core},
            )
        else:
            def step(c, carry):
                for a in range(2):
                    add_into(own.at[slot, a, side, c], mid.at[slot, a, c], dtype)
                return carry

            lax.fori_loop(0, n_clip, step, 0)
            away = send(own.at[slot, 1 - head, side], late.at[slot], i, 3, {"head": 1 - head})
        away.start()
        started.append(away)
        thirds[i] = away

    def third(i):
        kind, slot = pieces[i][:2]
        own, _, _, late, last = kinds[kind]
        thirds[i].wait_recv()
        dtype = own.dtype

        def step(c, carry):
            add_into(own.at[slot, head, side, c], late.at[slot, c], dtype)
            return carry

        lax.fori_loop(0, n_clip, step, 0)
        fourths[i] = []
        for d in range(1, n_clip):
            there = lax.rem(clip + d, n_clip)
            away = send(
                own.at[slot, head, side, there], last.at[slot, d - 1], i, 3 + d, {"clip": there}
            )
            away.start()
            started.append(away)
            fourths[i].append(away)

    def fourth(i):
        kind, slot, _, _, size, out_at = pieces[i]
        own, last = kinds[kind][0], kinds[kind][4]
        total = own[slot, head, side, clip].astype(F32)
        for d in range(1, n_clip):
            fourths[i][d - 1].wait_recv()
            total = total + last[slot, d - 1].astype(F32)
        outs[kind][:, out_at:out_at + size] = total

    steps = (first, second, third, fourth)
    for wave in range(len(pieces) + 3):
        for back, stage in enumerate(steps):
            if 0 <= wave - back < len(pieces):
                stage(wave - back)
    for away in started:
        away.wait_send()


def scatter_grads(grads, vectors, name_id):
    n_head, n_clip, sides, _, strip, _ = grads[0].shape
    pieces = [(1, 0, len(grads), 0, vectors.shape[5], 0)]
    chunk = min(g.shape[5] for g in grads)
    at_out = 0
    for j, g in enumerate(grads):
        for at in range(0, g.shape[5], chunk):
            pieces.append((0, len(pieces) - 1, j, at, chunk, at_out))
            at_out += chunk
    n_low = len(pieces) - 1

    def buffers(n, rows, cols, dtype):
        return [
            pltpu.VMEM((n, n_head, sides, n_clip, rows, cols), dtype),
            pltpu.VMEM((n, n_head, sides, n_clip, rows, cols), dtype),
            pltpu.VMEM((n, 2, n_clip, rows, cols), dtype),
            pltpu.VMEM((n, n_clip, rows, cols), dtype),
            pltpu.VMEM((n, n_clip - 1, rows, cols), dtype),
        ]

    any_spec = pl.BlockSpec(memory_space=pl.ANY)
    vmem = pl.BlockSpec(memory_space=pltpu.VMEM)
    n_src = len(grads) + 1
    return pl.pallas_call(
        functools.partial(scatter_kernel, n_clip, tuple(pieces), n_src),
        out_shape=(
            jax.ShapeDtypeStruct((strip, at_out), F32),
            jax.ShapeDtypeStruct(vectors.shape[4:], F32),
        ),
        in_specs=[any_spec] * n_src,
        out_specs=(vmem, vmem),
        scratch_shapes=buffers(n_low, strip, chunk, BF) + buffers(1, *vectors.shape[4:], F32)
        + [pltpu.SemaphoreType.DMA((2, len(pieces), n_clip + 5))],
        compiler_params=pltpu.CompilerParams(
            collective_id=name_id, has_side_effects=True, vmem_limit_bytes=40 * 1024 * 1024
        ),
        name="scatter_grads",
    )(*grads, vectors)


def product(form, left, right):
    return jnp.einsum(form, left, right, preferred_element_type=F32)


def norm_stats(values):
    mean = jnp.mean(values, axis=-1, keepdims=True)
    centred = values - mean
    spread = jnp.mean(centred * centred, axis=-1, keepdims=True)
    rate = lax.rsqrt(spread + NORM_EPS)
    return centred * rate, rate


def norm_back(unit, rate, gain, grad_normed):
    grad_gain = jnp.sum(grad_normed * unit, axis=0)
    grad_shift = jnp.sum(grad_normed, axis=0)
    scaled = grad_normed * gain
    inner = jnp.mean(scaled * unit, axis=-1, keepdims=True)
    outer = jnp.mean(scaled, axis=-1, keepdims=True)
    return rate * (scaled - outer - unit * inner), grad_gain, grad_shift


def project_in(normed, weights, bias):
    groups, _, triple = weights.shape
    width = triple // 3
    full = jnp.stack([bias[:, 0], jnp.zeros_like(bias[:, 0]), bias[:, 1]], axis=1)
    rows = product("nd,hdk->hnk", normed, weights) + full.reshape(groups, 1, triple)
    return rows.astype(BF).reshape(groups, normed.shape[0], 3, width)


def split_heads(merged, lead):
    groups = merged.shape[0]
    shaped = merged.reshape((groups,) + lead + (3, merged.shape[-1] // HEAD_DIM, HEAD_DIM))
    return shaped[..., 0, :, :], shaped[..., 1, :, :], shaped[..., 2, :, :]


def attend(merged, lead):
    queries, keys, values = split_heads(merged, lead)
    scores = product("gbqje,gbkje->gbjqk", queries, keys) * HEAD_DIM ** (-0.5)
    weights = jnp.exp(scores - jnp.max(scores, axis=-1, keepdims=True))
    probs = weights / jnp.sum(weights, axis=-1, keepdims=True)
    mixed = product("gbjqk,gbkje->gbqje", probs.astype(BF), values).astype(BF)
    return mixed.reshape(merged.shape[0], merged.shape[1], merged.shape[3]), probs


def attend_back(merged, probs, grad_mixed, lead):
    queries, keys, values = split_heads(merged, lead)
    grad_heads = grad_mixed.reshape(queries.shape)
    grad_values = product("gbjqk,gbqje->gbkje", probs.astype(BF), grad_heads)
    grad_probs = product("gbqje,gbkje->gbjqk", grad_heads, values)
    grad_scores = probs * (grad_probs - jnp.sum(probs * grad_probs, axis=-1, keepdims=True))
    grad_scores = grad_scores.astype(BF)
    scale = HEAD_DIM ** (-0.5)
    grad_queries = product("gbjqk,gbkje->gbqje", grad_scores, keys) * scale
    grad_keys = product("gbjqk,gbqje->gbkje", grad_scores, queries) * scale
    stacked = jnp.stack([grad_queries, grad_keys, grad_values], axis=3).astype(BF)
    return stacked.reshape(merged.shape)


def to_places(rows, count):
    frames, places, width = rows.shape
    share = -(-places // count)
    padded = jnp.pad(rows, ((0, 0), (0, share * count - places), (0, 0)))
    cut = padded.reshape(frames, count, share, width).transpose(1, 0, 2, 3)
    moved = lax.all_to_all(cut, PLACE_AXES, split_axis=0, concat_axis=0, tiled=True)
    return moved.reshape(count * frames, share, width)


def to_frames(rows, count, places):
    total, share, width = rows.shape
    frames = total // count
    cut = rows.reshape(count, frames, share, width)
    moved = lax.all_to_all(cut, PLACE_AXES, split_axis=0, concat_axis=0, tiled=True)
    back = moved.transpose(1, 0, 2, 3).reshape(frames, count * share, width)
    return back[:, :places]


def gather(block):
    return lax.all_gather(block, SHARDS, axis=0, tiled=False)


def body(
    inputs,
    space_gain,
    space_shift,
    space_proj,
    space_bias,
    space_out,
    space_out_bias,
    time_gain,
    time_shift,
    time_proj,
    time_bias,
    time_out,
    time_out_bias,
    dense_gain,
    dense_shift,
    dense_in,
    dense_bias,
    dense_out,
    dense_out_bias,
    cotangent,
):
    n_head = lax.axis_size("head")
    n_own = lax.axis_size("clip") * lax.axis_size("seq")
    count = lax.axis_size("seq") * n_head
    here = lax.axis_index("head")
    _, held, places, width = inputs.shape
    frames = held // n_head
    strip = space_gain.shape[0]

    def block_of(proj, out):
        flat = proj.reshape(strip, -1).astype(BF)
        return jnp.concatenate([flat, out.astype(BF).T], axis=1)

    def whole(block):
        return gather(block).reshape(n_head, width, block.shape[1])

    space_all = whole(block_of(space_proj, space_out))
    time_all = whole(block_of(time_proj, time_out))
    dense_all = whole(block_of(dense_in, dense_out))
    part = space_out.shape[0]
    hidden = dense_out.shape[0]

    vectors = (
        space_gain, space_shift, space_out_bias, time_gain, time_shift, time_out_bias,
        dense_gain, dense_shift, dense_out_bias,
    )
    odd = (space_bias, time_bias, dense_bias)
    small = jnp.concatenate([v.reshape(-1) for v in vectors + odd]).astype(BF)
    small_all = gather(small).reshape(n_head, n_own, -1).astype(F32)
    whole_vectors = []
    for i in range(len(vectors)):
        whole_vectors.append(small_all[0, :, i * strip:(i + 1) * strip].reshape(width))
    at = len(vectors) * strip
    sizes = [v.size for v in odd]
    bias_s = small_all[:, :, at:at + sizes[0]]
    bias_t = small_all[:, :, at + sizes[0]:at + sizes[0] + sizes[1]]
    bias_d = small_all[:, :, at + sizes[0] + sizes[1]:]

    def rows_bias(flat, shape):
        lines, lanes = shape[:-1], shape[-1]
        count_lines = 1
        for n in lines:
            count_lines *= n
        spread = flat.reshape(n_head, n_own, count_lines, lanes).transpose(0, 2, 1, 3)
        return spread.reshape(n_head, lines[0], -1)

    bias_s = rows_bias(bias_s, space_bias.shape)
    bias_t = rows_bias(bias_t, time_bias.shape)
    bias_d = rows_bias(bias_d, dense_bias.shape).reshape(n_head, 1, hidden)
    (g_s, b_s, ob_s, g_t, b_t, ob_t, g_d, b_d, ob_d) = whole_vectors

    own = lax.dynamic_slice_in_dim(inputs[0], here * frames, frames, axis=0)
    own = own.reshape(frames * places, width)
    cot = lax.dynamic_slice_in_dim(cotangent[0], here * frames, frames, axis=0)
    cot = cot.reshape(frames * places, width)

    proj_s, out_s = space_all[..., :3 * part], space_all[..., 3 * part:]
    proj_t, out_t = time_all[..., :3 * part], time_all[..., 3 * part:]
    in_d, out_d = dense_all[..., :hidden], dense_all[..., hidden:]

    unit_s, rate_s = norm_stats(own)
    normed_s = (unit_s * g_s + b_s).astype(BF)
    merged_s = project_in(normed_s, proj_s, bias_s)
    mixed_s, probs_s = attend(merged_s, (frames, places))
    after_space = own + product("hnw,hdw->nd", mixed_s, out_s) + ob_s

    unit_t, rate_t = norm_stats(after_space)
    normed_t = (unit_t * g_t + b_t).astype(BF)
    rows_t = to_places(normed_t.reshape(frames, places, width), count)
    total_frames, share = rows_t.shape[:2]
    rows_t = rows_t.transpose(1, 0, 2).reshape(-1, width)
    lead_t = (share, total_frames)
    merged_t = project_in(rows_t, proj_t, bias_t)
    mixed_t, probs_t = attend(merged_t, lead_t)
    branch_t = product("hnw,hdw->nd", mixed_t, out_t).astype(BF)
    branch_t = to_frames(branch_t.reshape(share, total_frames, width).transpose(1, 0, 2), count, places)
    after_time = after_space + branch_t.reshape(-1, width).astype(F32) + ob_t

    unit_d, rate_d = norm_stats(after_time)
    normed_d = (unit_d * g_d + b_d).astype(BF)
    pre = product("nd,hdk->hnk", normed_d, in_d) + bias_d
    act = jax.nn.gelu(pre, approximate=False).astype(BF)
    result = after_time + product("hnk,hdk->nd", act, out_d) + ob_d

    grad_ob_d = jnp.sum(cot, axis=0)
    low_d = cot.astype(BF)
    grad_out_d = product("nd,hnk->hdk", low_d, act)
    grad_act = product("nd,hdk->hnk", low_d, out_d).astype(BF).astype(F32)
    _, pull = jax.vjp(lambda v: jax.nn.gelu(v, approximate=False), pre)
    grad_pre = pull(grad_act)[0]
    grad_bias_d = jnp.sum(grad_pre, axis=1)
    low_pre = grad_pre.astype(BF)
    grad_in_d = product("nd,hnk->hdk", normed_d, low_pre)
    grad_normed = product("hnk,hdk->nd", low_pre, in_d)
    grad_v, grad_g_d, grad_b_d = norm_back(unit_d, rate_d, g_d, grad_normed)
    stream_t = cot + grad_v
    dense_grads = jnp.concatenate([grad_in_d.astype(BF), grad_out_d.astype(BF)], axis=2)
    stream_t, dense_grads = lax.optimization_barrier((stream_t, dense_grads))

    grad_ob_t = jnp.sum(stream_t, axis=0)
    low_t = to_places(stream_t.astype(BF).reshape(frames, places, width), count)
    low_t = low_t.transpose(1, 0, 2).reshape(-1, width)
    grad_out_t = product("nd,hnw->hdw", low_t, mixed_t)
    grad_mixed = product("nd,hdw->hnw", low_t, out_t).astype(BF)
    grad_merged_t = attend_back(merged_t, probs_t, grad_mixed, lead_t)
    sums_t = jnp.sum(grad_merged_t.astype(F32), axis=1)
    flat_t = grad_merged_t.reshape(n_head, -1, 3 * part)
    grad_proj_t = product("nd,hnk->hdk", rows_t, flat_t)
    grad_rows = product("hnk,hdk->nd", flat_t, proj_t).astype(BF)
    grad_rows = to_frames(grad_rows.reshape(share, total_frames, width).transpose(1, 0, 2), count, places)
    grad_v, grad_g_t, grad_b_t = norm_back(unit_t, rate_t, g_t, grad_rows.reshape(-1, width).astype(F32))
    stream_s = stream_t + grad_v

    grad_ob_s = jnp.sum(stream_s, axis=0)
    low_s = stream_s.astype(BF)
    grad_out_s = product("nd,hnw->hdw", low_s, mixed_s)
    grad_mixed = product("nd,hdw->hnw", low_s, out_s).astype(BF)
    grad_merged_s = attend_back(merged_s, probs_s, grad_mixed, (frames, places))
    sums_s = jnp.sum(grad_merged_s.astype(F32), axis=1)
    flat_s = grad_merged_s.reshape(n_head, -1, 3 * part)
    grad_proj_s = product("nd,hnk->hdk", normed_s, flat_s)
    grad_rows = product("hnk,hdk->nd", flat_s, proj_s)
    grad_v, grad_g_s, grad_b_s = norm_back(unit_s, rate_s, g_s, grad_rows)
    input_own = stream_s + grad_v

    vector_grads = jnp.stack([
        grad_g_s, grad_b_s, grad_ob_s, grad_g_t, grad_b_t, grad_ob_t, grad_g_d, grad_b_d, grad_ob_d,
    ])
    vector_grads = vector_grads.reshape(-1, n_own, strip).transpose(1, 0, 2).reshape(1, n_own, -1)

    def spread_bias(rows, shape):
        lanes = shape[-1]
        cut = rows.reshape(n_head, -1, n_own, lanes).transpose(0, 2, 1, 3)
        return cut.reshape(n_head, n_own, -1)

    small_grads = jnp.concatenate([
        jnp.broadcast_to(vector_grads, (n_head,) + vector_grads.shape[1:]),
        spread_bias(sums_s[:, ::2], space_bias.shape),
        spread_bias(sums_t[:, ::2], time_bias.shape),
        spread_bias(grad_bias_d, dense_bias.shape),
    ], axis=2)

    def owners(grad):
        mine = lax.psum_scatter(
            grad.astype(BF).reshape(n_head * width, -1), SHARDS, scatter_dimension=0, tiled=True
        )
        return mine.astype(F32)

    own_d = owners(dense_grads)
    if strip % 16 == 0:
        blocks = (n_head, lax.axis_size("clip"), 2, 2)
        low = [
            g.astype(BF).reshape(blocks + (strip, -1))
            for g in (grad_proj_s, grad_out_s, grad_proj_t, grad_out_t)
        ]
        room = -small_grads.shape[2] % 1024
        tiles = jnp.pad(small_grads, ((0, 0), (0, 0), (0, room))).reshape(blocks + (-1, 128))
        large, mine = scatter_grads(low, tiles, 1)
        mine = mine.reshape(-1)
        step = 4 * part
        own_s, own_t = large[:, :step], large[:, step:]
    else:
        own_s = owners(jnp.concatenate([grad_proj_s, grad_out_s], axis=2))
        own_t = owners(jnp.concatenate([grad_proj_t, grad_out_t], axis=2))
        mine = lax.psum_scatter(small_grads, ("clip", "seq"), scatter_dimension=1, tiled=True)
        mine = lax.dynamic_index_in_dim(lax.psum(mine, "head"), here, axis=0, keepdims=False)[0]
    got = [mine[i * strip:(i + 1) * strip] for i in range(9)]
    odd_got = []
    at = 9 * strip
    for v in odd:
        odd_got.append(mine[at:at + v.size].reshape(v.shape))
        at += v.size

    def share_rows(rows):
        low = rows.astype(BF).reshape(frames, places, width)
        both_rows = lax.all_gather(low, "head", axis=0, tiled=True)
        return both_rows.astype(F32)[None]

    return (
        share_rows(result),
        share_rows(input_own),
        got[0],
        got[1],
        own_s[:, :3 * part].reshape(space_proj.shape),
        odd_got[0],
        own_s[:, 3 * part:].T,
        got[2],
        got[3],
        got[4],
        own_t[:, :3 * part].reshape(time_proj.shape),
        odd_got[1],
        own_t[:, 3 * part:].T,
        got[5],
        got[6],
        got[7],
        own_d[:, :hidden],
        odd_got[2],
        own_d[:, hidden:].T,
        got[8],
    )


def solution(mesh):
    both = ("clip", "seq")
    rows = P("clip", "seq", None, None)
    vec = P(both)
    weights = (
        vec, vec, P(both, None, "head"), P(None, "head", both), P("head", both), vec,
        vec, vec, P(both, None, "head"), P(None, "head", both), P("head", both), vec,
        vec, vec, P(both, "head"), P("head", both), P("head", both), vec,
    )

    return jax.shard_map(
        body,
        mesh=mesh,
        in_specs=(rows,) + weights + (rows,),
        out_specs=(rows, rows) + weights,
        check_vma=False,
    )
```
